32 devices in a mesh: dp: 8 (over z, y), ep: 4 (over x, core).
Axes of the slice: x: 2, y: 2, z: 4, core: 2. Of those that a mesh axis runs over, the one named last changes fastest.
Arguments:
- x: bfloat16 [65536, 768], P(('dp', 'ep'))
- gy: bfloat16 [65536, 768], P(('dp', 'ep'))
- idx: int32 [65536], P(('dp', 'ep'))
- w_gate: bfloat16 [768, 8], replicated
- w_up: bfloat16 [8, 768, 3072], P('ep')
- w_down: bfloat16 [8, 3072, 768], P('ep')
Outputs:
- output 1: bfloat16 [65536, 768], P(('dp', 'ep'))
- output 2: bfloat16 [65536, 768], P(('dp', 'ep'))
- output 3: float32 [8, 768, 3072], P('ep')
- output 4: float32 [8, 3072, 768], P('ep')
- output 5: float32 [768, 8], replicated
All inputs are finite; a program needn't handle non-finite values.
Results may differ from the reference program's by a relative error of at most 0.00594816.
Values are sent between devices in bfloat16 or wider.
A program may use at most 1 GiB of HBM per device.

```python
import functools
import jax
import jax.numpy as jnp
from jax import lax

D_MODEL = 768
D_FF = 3072
N_EXPERTS = 8
TOKENS_DEV = 2048
N_DEVICES = 32
TILE_ROWS = 128
N_TOKENS = N_DEVICES * TOKENS_DEV
CAP_ROWS = 4 * TOKENS_DEV // N_EXPERTS
N_TILES = N_TOKENS // TILE_ROWS + N_EXPERTS


def count_profile():
    hot_experts = max(1, N_EXPERTS // 16)
    cold_experts = N_EXPERTS - hot_experts
    rest_rows = TOKENS_DEV - hot_experts * CAP_ROWS
    base_rows = rest_rows // cold_experts
    extra_rows = rest_rows % cold_experts
    return [CAP_ROWS] * hot_experts + [base_rows + 1] * extra_rows + [base_rows] * (cold_experts - extra_rows)


def draw_routing(route_key):
    profile = count_profile()
    rank_table = jnp.array([rank_id for rank_id in range(N_EXPERTS) for copy_num in range(profile[rank_id])], jnp.int32)

    def one_device(dev_key):
        perm_key, shuffle_key = jax.random.split(dev_key)
        expert_perm = jax.random.permutation(perm_key, N_EXPERTS).astype(jnp.int32)
        return jax.random.permutation(shuffle_key, expert_perm[rank_table])

    return jax.vmap(one_device)(jax.random.split(route_key, N_DEVICES)).reshape(N_TOKENS)


def setup_inputs(seed: int = 0) -> dict:
    root_key = jax.random.key(seed)
    k_x, k_gy, k_gate, k_up, k_down, k_route = jax.random.split(root_key, 6)
    x = jax.random.normal(k_x, (N_TOKENS, D_MODEL), jnp.float32).astype(jnp.bfloat16)
    gy = jax.random.normal(k_gy, (N_TOKENS, D_MODEL), jnp.float32).astype(jnp.bfloat16)
    w_gate = (jax.random.normal(k_gate, (D_MODEL, N_EXPERTS), jnp.float32) * D_MODEL ** -0.5).astype(jnp.bfloat16)
    w_up = (jax.random.normal(k_up, (N_EXPERTS, D_MODEL, D_FF), jnp.float32) * D_MODEL ** -0.5).astype(jnp.bfloat16)
    w_down = (jax.random.normal(k_down, (N_EXPERTS, D_FF, D_MODEL), jnp.float32) * D_FF ** -0.5).astype(jnp.bfloat16)
    idx = draw_routing(k_route)
    return {'x': x, 'gy': gy, 'idx': idx, 'w_gate': w_gate, 'w_up': w_up, 'w_down': w_down}


def tile_pass(w_up, w_down, grad_carry, tile_in):
    grad_up, grad_down = grad_carry
    tok_rows, d_out, expert = tile_in
    up_mat = w_up[expert]
    down_mat = w_down[expert]
    pre_act = jnp.dot(tok_rows, up_mat, preferred_element_type=jnp.float32)
    hid_full, gelu_back = jax.vjp(jax.nn.gelu, pre_act)
    hidden = hid_full.astype(jnp.bfloat16)
    y_rows = jnp.dot(hidden, down_mat, preferred_element_type=jnp.float32).astype(jnp.bfloat16)
    d_hidden = jnp.dot(d_out, down_mat.T, preferred_element_type=jnp.float32)
    d_pre = gelu_back(d_hidden)[0].astype(jnp.bfloat16)
    grad_down = grad_down.at[expert].add(jnp.dot(hidden.T, d_out, preferred_element_type=jnp.float32))
    grad_up = grad_up.at[expert].add(jnp.dot(tok_rows.T, d_pre, preferred_element_type=jnp.float32))
    d_rows = jnp.dot(d_pre, up_mat.T, preferred_element_type=jnp.float32).astype(jnp.bfloat16)
    return (grad_up, grad_down), (y_rows, d_rows)


def reference(x, gy, idx, w_gate, w_up, w_down):
    onehot = idx[:, None] == jnp.arange(N_EXPERTS, dtype=jnp.int32)[None, :]
    router_logit = jnp.dot(x, w_gate, preferred_element_type=jnp.float32)
    router_prob = jax.nn.softmax(router_logit, axis=-1)
    gate_val = N_EXPERTS * jnp.sum(jnp.where(onehot, router_prob, 0.0), axis=1)
    expert_count = jnp.sum(onehot, axis=0, dtype=jnp.int32)
    sort_order = jnp.argsort(idx, stable=True)
    sorted_pos = jnp.argsort(sort_order)
    expert_start = jnp.cumsum(expert_count) - expert_count
    tile_count = (expert_count + TILE_ROWS - 1) // TILE_ROWS * TILE_ROWS
    tile_end = jnp.cumsum(tile_count)
    tile_start = tile_end - tile_count
    row_pos = tile_start[idx] + sorted_pos - expert_start[idx]
    tile_first = jnp.arange(N_TILES, dtype=jnp.int32) * TILE_ROWS
    tile_expert = jnp.minimum(jnp.sum(tile_end[None, :] <= tile_first[:, None], axis=1, dtype=jnp.int32), N_EXPERTS - 1)
    gy_full = gy.astype(jnp.float32)
    dy_tok = (gate_val[:, None] * gy_full).astype(jnp.bfloat16)
    rows_buf = jnp.zeros((N_TILES * TILE_ROWS, D_MODEL), x.dtype).at[row_pos].set(x)
    dy_buf = jnp.zeros((N_TILES * TILE_ROWS, D_MODEL), dy_tok.dtype).at[row_pos].set(dy_tok)
    grad_init = (jnp.zeros((N_EXPERTS, D_MODEL, D_FF), jnp.float32), jnp.zeros((N_EXPERTS, D_FF, D_MODEL), jnp.float32))
    tiles_in = (rows_buf.reshape(N_TILES, TILE_ROWS, D_MODEL), dy_buf.reshape(N_TILES, TILE_ROWS, D_MODEL), tile_expert)
    grads, tile_out = lax.scan(functools.partial(tile_pass, w_up, w_down), grad_init, tiles_in)
    grad_up, grad_down = grads
    y_tok = tile_out[0].reshape(N_TILES * TILE_ROWS, D_MODEL)[row_pos]
    dx_expert = tile_out[1].reshape(N_TILES * TILE_ROWS, D_MODEL)[row_pos]
    moe_out = (gate_val[:, None] * y_tok.astype(jnp.float32)).astype(jnp.bfloat16)
    d_gate = jnp.sum(gy_full * y_tok.astype(jnp.float32), axis=1)
    d_logit = ((d_gate * gate_val)[:, None] * (onehot.astype(jnp.float32) - router_prob)).astype(jnp.bfloat16)
    dx_router = jnp.dot(d_logit, w_gate.T, preferred_element_type=jnp.float32)
    grad_x = (dx_expert.astype(jnp.float32) + dx_router).astype(jnp.bfloat16)
    grad_gate = jnp.dot(x.T, d_logit, preferred_element_type=jnp.float32)
    return (moe_out, grad_x, grad_up, grad_down, grad_gate)
```

```python
import jax
import jax.numpy as jnp
from jax import lax
from jax.sharding import PartitionSpec as P

PAD_FACTOR = 4
ROW_SIXTEENTHS = (3, 6, 10, 13, 16)


def solution(mesh):
    ep_size = mesh.shape['ep']
    dp_size = mesh.shape['dp']
    tok_spec = P(('dp', 'ep'), None)
    idx_spec = P(('dp', 'ep'))
    rep_spec = P(None, None)
    exp_spec = P('ep', None, None)

    def swap(value, bit):
        return lax.ppermute(value, 'ep', [(i, i ^ bit) for i in range(ep_size)])

    def expert_pass(rows):
        def run(x_all, dy_all, src, used, w1, w2):
            total = src.shape[0]
            pick = src[:rows]
            xs = x_all[pick]
            ds = jnp.where(jnp.arange(rows, dtype=jnp.int32)[:, None] < used, dy_all[pick], jnp.zeros((), dy_all.dtype))
            pre_act = jnp.dot(xs, w1, preferred_element_type=jnp.float32)
            hid_full, gelu_back = jax.vjp(jax.nn.gelu, pre_act)
            hidden = hid_full.astype(jnp.bfloat16)
            d_hidden = jnp.einsum('kd,fd->kf', ds, w2, preferred_element_type=jnp.float32)
            d_pre = gelu_back(d_hidden)[0].astype(jnp.bfloat16)
            grad_down = jnp.einsum('kf,kd->fd', hidden, ds, preferred_element_type=jnp.float32).astype(jnp.bfloat16)
            grad_up = jnp.einsum('kd,kf->df', xs, d_pre, preferred_element_type=jnp.float32).astype(jnp.bfloat16)
            y_rows = jnp.dot(hidden, w2, preferred_element_type=jnp.float32).astype(jnp.bfloat16)
            d_rows = jnp.einsum('kf,df->kd', d_pre, w1, preferred_element_type=jnp.float32).astype(jnp.bfloat16)
            tail = ((0, total - rows), (0, 0))
            return jnp.pad(y_rows, tail), jnp.pad(d_rows, tail), grad_up, grad_down

        return run

    def scatter_dp(part, my_dp):
        rows, cols = part.shape
        pieces = part.reshape(dp_size, rows // dp_size, cols)
        half = dp_size // 2
        got = [lax.dynamic_index_in_dim(pieces, my_dp, 0, keepdims=False)]
        for hop in range(1, dp_size):
            far, flip = hop // 2, hop % 2
            pairs = [(i, (i // 2 + far) % half * 2 + (i % 2 + flip) % 2) for i in range(dp_size)]
            target = (my_dp // 2 + far) % half * 2 + (my_dp + flip) % 2
            piece = lax.dynamic_index_in_dim(pieces, target, 0, keepdims=False)
            got.append(lax.ppermute(piece, 'dp', pairs))
        return got

    def gather_dp(got):
        total = got[0].astype(jnp.float32)
        for piece in got[1:]:
            total = total + piece.astype(jnp.float32)
        return lax.all_gather(total.astype(jnp.bfloat16), 'dp', axis=0, tiled=True)

    def local_step(x_loc, gy_loc, idx_loc, w_gate, w_up, w_down):
        tok_count, _ = x_loc.shape
        n_experts = w_gate.shape[1]
        local_experts = w_up.shape[0]
        max_rows = ep_size * PAD_FACTOR * tok_count // n_experts
        sizes = [max_rows * part // 16 for part in ROW_SIXTEENTHS]
        me = lax.axis_index('ep')
        my_dp = lax.axis_index('dp')
        onehot = idx_loc[:, None] == jnp.arange(n_experts, dtype=jnp.int32)[None, :]

        router_logit = jnp.dot(x_loc, w_gate, preferred_element_type=jnp.float32)
        router_prob = jax.nn.softmax(router_logit, axis=-1)
        gate_val = n_experts * jnp.sum(jnp.where(onehot, router_prob, 0.0), axis=1)
        gy_full = gy_loc.astype(jnp.float32)

        def dispatch(tok_rows):
            far_rows = swap(tok_rows, 2)
            near_rows = swap(tok_rows, 1)
            return jnp.concatenate([tok_rows, near_rows, far_rows, swap(far_rows, 1)], axis=0)

        x_all = dispatch(x_loc)
        gy_all = dispatch(gy_loc)

        def by_distance(value):
            group = lax.all_gather(value, 'ep')
            return [lax.dynamic_index_in_dim(group, me ^ j, 0, keepdims=False) for j in range(ep_size)]

        idx_rel = by_distance(idx_loc)
        gate_all = jnp.concatenate(by_distance(gate_val))
        dy_all = (gate_all[:, None] * gy_all.astype(jnp.float32)).astype(jnp.bfloat16)
        slot_exp = jnp.concatenate(idx_rel) - me * local_experts
        mine = (slot_exp >= 0) & (slot_exp < local_experts)
        key = jnp.where(mine, slot_exp, local_experts)
        order = jnp.argsort(key, stable=True).astype(jnp.int32)
        place = jnp.argsort(order).astype(jnp.int32)
        used = jnp.sum(key[:, None] == jnp.arange(local_experts, dtype=jnp.int32)[None, :], axis=0, dtype=jnp.int32)
        begin = jnp.cumsum(used) - used
        shift = sum(jnp.where(key == l, l * max_rows - begin[l], 0) for l in range(local_experts))
        slot = jnp.where(mine, place + shift, 0)
        order, slot = lax.optimization_barrier((order, slot))

        y_parts, d_parts, ups, downs = [], [], [], []
        for l in range(local_experts):
            src = lax.dynamic_slice(order, (begin[l],), (max_rows,))
            which = sum((used[l] > size).astype(jnp.int32) for size in sizes[:-1])
            y_rows, d_rows, grad_up, grad_down = lax.switch(
                which, [expert_pass(size) for size in sizes], x_all, dy_all, src, used[l], w_up[l], w_down[l])
            if l > 0:
                (y_rows, d_rows, grad_up, grad_down), downs[-1], ups[-1] = lax.optimization_barrier(
                    ((y_rows, d_rows, grad_up, grad_down), downs[-1], ups[-1]))
            y_parts.append(y_rows)
            d_parts.append(d_rows)
            downs.append(scatter_dp(grad_down, my_dp))
            ups.append(scatter_dp(grad_up, my_dp))

        def place_rows(parts):
            table = jnp.concatenate(parts, axis=0)
            slots = slot.reshape(ep_size, tok_count)
            out_rows = table[jnp.concatenate([slots[3], slots[1]])]
            keep_rows = table[jnp.concatenate([slots[2], slots[0]])]
            near_far = swap(out_rows[:tok_count], 1)
            near_own = swap(out_rows[tok_count:], 1)
            far_mine = (idx_rel[2] // local_experts == me)[:, None]
            return jnp.where(far_mine, keep_rows[:tok_count], near_far), keep_rows[tok_count:], near_own

        def combine(far_out, keep_own, near_own):
            owner = (idx_loc // local_experts)[:, None]
            return jnp.where(owner == me, keep_own, jnp.where(owner == (me ^ 1), near_own, swap(far_out, 2)))

        y_sent = place_rows(y_parts)
        d_sent = place_rows(d_parts)
        y_sent, d_sent, downs[-1], ups[-1] = lax.optimization_barrier((y_sent, d_sent, downs[-1], ups[-1]))
        y_tok = combine(*y_sent).astype(jnp.float32)
        dx_expert = combine(*d_sent).astype(jnp.float32)
        moe_out = (gate_val[:, None] * y_tok).astype(jnp.bfloat16)
        d_gate = jnp.sum(gy_full * y_tok, axis=1)
        d_logit = ((d_gate * gate_val)[:, None] * (onehot.astype(jnp.float32) - router_prob)).astype(jnp.bfloat16)
        dx_router = jnp.einsum('te,de->td', d_logit, w_gate, preferred_element_type=jnp.float32)
        grad_x = (dx_expert + dx_router).astype(jnp.bfloat16)
        grad_gate = jnp.einsum('td,te->de', x_loc, d_logit, preferred_element_type=jnp.float32)
        grad_gate = lax.psum(grad_gate, ('dp', 'ep'))
        grad_down = jnp.stack([gather_dp(got) for got in downs]).astype(jnp.float32)
        grad_up = jnp.stack([gather_dp(got) for got in ups]).astype(jnp.float32)
        return moe_out, grad_x, grad_up, grad_down, grad_gate

    return jax.shard_map(local_step, mesh=mesh, in_specs=(tok_spec, tok_spec, idx_spec, rep_spec, exp_spec, exp_spec), out_specs=(tok_spec, tok_spec, exp_spec, exp_spec, rep_spec), check_vma=False)
```

```python
import jax
import jax.numpy as jnp
from jax import lax
from jax.sharding import PartitionSpec as P

PAD_FACTOR = 4
ROW_SIXTEENTHS = (3, 6, 10, 13, 16)


def solution(mesh):
    ep_size = mesh.shape['ep']
    dp_size = mesh.shape['dp']
    tok_spec = P(('dp', 'ep'), None)
    idx_spec = P(('dp', 'ep'))
    rep_spec = P(None, None)
    exp_spec = P('ep', None, None)

    def swap(value, bit):
        return lax.ppermute(value, 'ep', [(i, i ^ bit) for i in range(ep_size)])

    def expert_pass(rows):
        def run(x_all, dy_all, src, used, w1, w2):
            total = src.shape[0]
            pick = src[:rows]
            xs = x_all[pick]
            ds = jnp.where(jnp.arange(rows, dtype=jnp.int32)[:, None] < used, dy_all[pick], jnp.zeros((), dy_all.dtype))
            pre_act = jnp.dot(xs, w1, preferred_element_type=jnp.float32)
            hid_full, gelu_back = jax.vjp(jax.nn.gelu, pre_act)
            hidden = hid_full.astype(jnp.bfloat16)
            d_hidden = jnp.einsum('kd,fd->kf', ds, w2, preferred_element_type=jnp.float32)
            d_pre = gelu_back(d_hidden)[0].astype(jnp.bfloat16)
            grad_down = jnp.einsum('kf,kd->fd', hidden, ds, preferred_element_type=jnp.float32).astype(jnp.bfloat16)
            grad_up = jnp.einsum('kd,kf->df', xs, d_pre, preferred_element_type=jnp.float32).astype(jnp.bfloat16)
            y_rows = jnp.dot(hidden, w2, preferred_element_type=jnp.float32).astype(jnp.bfloat16)
            d_rows = jnp.einsum('kf,df->kd', d_pre, w1, preferred_element_type=jnp.float32).astype(jnp.bfloat16)
            tail = ((0, total - rows), (0, 0))
            return jnp.pad(y_rows, tail), jnp.pad(d_rows, tail), grad_up, grad_down

        return run

    def scatter_dp(part, my_dp):
        rows, cols = part.shape
        pieces = part.reshape(dp_size, rows // dp_size, cols)
        half = dp_size // 2
        got = [lax.dynamic_index_in_dim(pieces, my_dp, 0, keepdims=False)]
        for hop in range(1, dp_size):
            far, flip = hop // 2, hop % 2
            pairs = [(i, (i // 2 + far) % half * 2 + (i % 2 + flip) % 2) for i in range(dp_size)]
            target = (my_dp // 2 + far) % half * 2 + (my_dp + flip) % 2
            piece = lax.dynamic_index_in_dim(pieces, target, 0, keepdims=False)
            got.append(lax.ppermute(piece, 'dp', pairs))
        return got

    def gather_dp(got):
        total = got[0].astype(jnp.float32)
        for piece in got[1:]:
            total = total + piece.astype(jnp.float32)
        return lax.all_gather(total.astype(jnp.bfloat16), 'dp', axis=0, tiled=True)

    def local_step(x_loc, gy_loc, idx_loc, w_gate, w_up, w_down):
        tok_count, _ = x_loc.shape
        n_experts = w_gate.shape[1]
        local_experts = w_up.shape[0]
        max_rows = ep_size * PAD_FACTOR * tok_count // n_experts
        sizes = [max_rows * part // 16 for part in ROW_SIXTEENTHS]
        me = lax.axis_index('ep')
        my_dp = lax.axis_index('dp')
        onehot = idx_loc[:, None] == jnp.arange(n_experts, dtype=jnp.int32)[None, :]

        router_logit = jnp.dot(x_loc, w_gate, preferred_element_type=jnp.float32)
        router_prob = jax.nn.softmax(router_logit, axis=-1)
        gate_val = n_experts * jnp.sum(jnp.where(onehot, router_prob, 0.0), axis=1)
        gy_full = gy_loc.astype(jnp.float32)

        def dispatch(tok_rows):
            far_rows = swap(tok_rows, 2)
            near_rows = swap(tok_rows, 1)
            return jnp.concatenate([tok_rows, near_rows, far_rows, swap(far_rows, 1)], axis=0)

        x_sent, gy_sent, idx_group = lax.optimization_barrier((x_loc, gy_loc, lax.all_gather(idx_loc, 'ep')))
        x_all = dispatch(x_sent)
        gy_all = dispatch(gy_sent)

        def by_distance(group):
            return [lax.dynamic_index_in_dim(group, me ^ j, 0, keepdims=False) for j in range(ep_size)]

        idx_rel = by_distance(idx_group)
        gate_all = jnp.concatenate(by_distance(lax.all_gather(gate_val, 'ep')))
        dy_all = (gate_all[:, None] * gy_all.astype(jnp.float32)).astype(jnp.bfloat16)
        slot_exp = jnp.concatenate(idx_rel) - me * local_experts
        mine = (slot_exp >= 0) & (slot_exp < local_experts)
        key = jnp.where(mine, slot_exp, local_experts)
        order = jnp.argsort(key, stable=True).astype(jnp.int32)
        place = jnp.argsort(order).astype(jnp.int32)
        used = jnp.sum(key[:, None] == jnp.arange(local_experts, dtype=jnp.int32)[None, :], axis=0, dtype=jnp.int32)
        begin = jnp.cumsum(used) - used
        shift = sum(jnp.where(key == l, l * max_rows - begin[l], 0) for l in range(local_experts))
        slot = jnp.where(mine, place + shift, 0)
        order, slot = lax.optimization_barrier((order, slot))

        y_parts, d_parts, ups, downs = [], [], [], []
        for l in range(local_experts):
            src = lax.dynamic_slice(order, (begin[l],), (max_rows,))
            which = sum((used[l] > size).astype(jnp.int32) for size in sizes[:-1])
            y_rows, d_rows, grad_up, grad_down = lax.switch(
                which, [expert_pass(size) for size in sizes], x_all, dy_all, src, used[l], w_up[l], w_down[l])
            if l > 0:
                (y_rows, d_rows, grad_up, grad_down), downs[-1], ups[-1] = lax.optimization_barrier(
                    ((y_rows, d_rows, grad_up, grad_down), downs[-1], ups[-1]))
            y_parts.append(y_rows)
            d_parts.append(d_rows)
            downs.append(scatter_dp(grad_down, my_dp))
            ups.append(scatter_dp(grad_up, my_dp))

        def place_rows(parts):
            table = jnp.concatenate(parts, axis=0)
            slots = slot.reshape(ep_size, tok_count)
            out_rows = table[jnp.concatenate([slots[3], slots[1]])]
            keep_rows = table[jnp.concatenate([slots[2], slots[0]])]
            near_far = swap(out_rows[:tok_count], 1)
            near_own = swap(out_rows[tok_count:], 1)
            far_mine = (idx_rel[2] // local_experts == me)[:, None]
            return jnp.where(far_mine, keep_rows[:tok_count], near_far), keep_rows[tok_count:], near_own

        def combine(far_out, keep_own, near_own):
            owner = (idx_loc // local_experts)[:, None]
            return jnp.where(owner == me, keep_own, jnp.where(owner == (me ^ 1), near_own, swap(far_out, 2)))

        y_sent = place_rows(y_parts)
        d_sent = place_rows(d_parts)
        y_sent, d_sent, downs[-1], ups[-1] = lax.optimization_barrier((y_sent, d_sent, downs[-1], ups[-1]))
        y_tok = combine(*y_sent).astype(jnp.float32)
        dx_expert = combine(*d_sent).astype(jnp.float32)
        moe_out = (gate_val[:, None] * y_tok).astype(jnp.bfloat16)
        d_gate = jnp.sum(gy_full * y_tok, axis=1)
        d_logit = ((d_gate * gate_val)[:, None] * (onehot.astype(jnp.float32) - router_prob)).astype(jnp.bfloat16)
        dx_router = jnp.einsum('te,de->td', d_logit, w_gate, preferred_element_type=jnp.float32)
        grad_x = (dx_expert + dx_router).astype(jnp.bfloat16)
        grad_gate = jnp.einsum('td,te->de', x_loc, d_logit, preferred_element_type=jnp.float32)
        grad_gate = lax.psum(grad_gate, ('dp', 'ep'))
        grad_down = jnp.stack([gather_dp(got) for got in downs]).astype(jnp.float32)
        grad_up = jnp.stack([gather_dp(got) for got in ups]).astype(jnp.float32)
        return moe_out, grad_x, grad_up, grad_down, grad_gate

    return jax.shard_map(local_step, mesh=mesh, in_specs=(tok_spec, tok_spec, idx_spec, rep_spec, exp_spec, exp_spec), out_specs=(tok_spec, tok_spec, exp_spec, exp_spec, rep_spec), check_vma=False)
```
